32 devices in a mesh: seg: 32 (over z, y, x, core).
Axes of the slice: x: 2, y: 2, z: 4, core: 2. Of those that a mesh axis runs over, the one named last changes fastest.
Arguments:
- tokens: bfloat16 [8192, 3584], P('seg'), may hold values from -6 to 6
- memory: bfloat16 [64, 3584], replicated, may hold values from -6 to 6
- norm_gain: float32 [3584], replicated, may hold values from 0.5 to 2
- post_gain: float32 [3584], replicated, may hold values from 0.5 to 2
- query_weight: bfloat16 [3584, 2048], P('seg'), may hold values from -0.09375 to 0.09375
- key_matrix: bfloat16 [3584, 1024], replicated, may hold values from -0.09375 to 0.09375
- value_matrix: bfloat16 [3584, 1024], replicated, may hold values from -0.09375 to 0.09375
- output_weight: bfloat16 [2048, 3584], P('seg'), may hold values from -0.125 to 0.125
- segment_weight: float32 [32], P('seg'), may hold values from 0.1 to 4
Outputs:
- token_out: bfloat16 [8192, 3584], P('seg')
- memory_out: bfloat16 [2048, 3584], P('seg')
- changes: float32 [3], replicated
The draws below stay inside these ranges and needn't reach their ends.
All inputs are finite; a program needn't handle non-finite values.
Results may differ from the reference program's by a relative error of at most 0.014.
Values may be sent and summed in bfloat16 or wider, within the bound.
A program may use at most 192 MiB of HBM per device.

```python
import math
import jax
import jax.numpy as jnp
from jax import lax

MODEL_WIDTH = 3584
HEAD_WIDTH = 256
HQ = 8
KEY_VALUE_HEADS = 4
MEM = 64
ITERS = 3
TOK_DEV = 256
SEGMENTS = 32
N_SEG = 32


def draw_segment_weight(key, part):
    ramp = jnp.arange(SEGMENTS).astype(jnp.float32) / max(SEGMENTS - 1, 1)
    level = jax.random.uniform(key, (SEGMENTS,), jnp.float32, 0.0, 1.0)
    return 0.1 + 0.3 * ramp + 3.6 * jnp.power(level, 8.0)


def level_of(stream_key, dims, split, low, high):
    factor_of = 1.0
    for dim, blocks in split:
        draws = jax.random.uniform(jax.random.fold_in(jax.random.fold_in(stream_key, 6), dim), (blocks,), jnp.float32, low / len(split), high / len(split))
        factor_of = factor_of * jnp.repeat(jnp.exp(draws), dims[dim] // blocks).reshape((-1,) + (1,) * (len(dims) - 1 - dim))
    return factor_of


def bell_draw(key, shape, spread, limit, shards=(), dtype=jnp.bfloat16):
    result = jax.random.normal(key, shape, jnp.float32) * spread
    if len(shards) > 0:
        result = level_of(key, shape, shards, -0.22, 0.18) * result
    return jnp.clip(result, min=-limit, max=limit).astype(dtype)


def setup_inputs(seed: int = 0) -> dict:
    key_list = jax.random.split(jax.random.key(seed), 10)
    return {
        "tokens": bell_draw(key_list[0], (SEGMENTS * TOK_DEV, MODEL_WIDTH), 1.0, 6.0, ((0, 32),)),
        "memory": bell_draw(key_list[1], (MEM, MODEL_WIDTH), 1.0, 6.0),
        "norm_gain": jnp.clip(jnp.exp(jax.random.uniform(key_list[2], (MODEL_WIDTH,), jnp.float32, math.log(0.5), math.log(2.0))), 0.5, 2.0),
        "post_gain": jnp.clip(jnp.exp(jax.random.uniform(key_list[3], (MODEL_WIDTH,), jnp.float32, math.log(0.5), math.log(2.0))), 0.5, 2.0),
        "query_weight": bell_draw(key_list[4], (MODEL_WIDTH, HQ * HEAD_WIDTH), MODEL_WIDTH ** -0.5, 0.09375, ((0, 32),)),
        "key_matrix": bell_draw(key_list[5], (MODEL_WIDTH, KEY_VALUE_HEADS * HEAD_WIDTH), MODEL_WIDTH ** -0.5, 0.09375),
        "value_matrix": bell_draw(key_list[6], (MODEL_WIDTH, KEY_VALUE_HEADS * HEAD_WIDTH), MODEL_WIDTH ** -0.5, 0.09375),
        "output_weight": bell_draw(key_list[7], (HQ * HEAD_WIDTH, MODEL_WIDTH), (HQ * HEAD_WIDTH) ** -0.5, 0.125, ((0, 32),)),
        "segment_weight": draw_segment_weight(jax.random.fold_in(key_list[9], 71), 0),
    }


eps = 1e-06

def prenorm(rows, gain):
    rows = rows.astype(jnp.float32)
    mean_sq = lax.optimization_barrier(jnp.mean(rows * rows, axis=-1, keepdims=True))
    return (rows / jnp.sqrt(mean_sq + eps) * gain).astype(jnp.bfloat16)

def attend(query_vectors, key_vectors, value_vectors, allowed):
    element_count = query_vectors.shape[0]
    feature_width = key_vectors.shape[0]
    query_heads_split = query_vectors.reshape(element_count, KEY_VALUE_HEADS, 2, HEAD_WIDTH).astype(jnp.float32)
    key_heads_split = key_vectors.reshape(feature_width, KEY_VALUE_HEADS, HEAD_WIDTH).astype(jnp.float32)
    value_heads_split = value_vectors.reshape(feature_width, KEY_VALUE_HEADS, HEAD_WIDTH).astype(jnp.float32)
    score = jnp.einsum('rgjd,kgd->gjrk', query_heads_split, key_heads_split)
    expo = jnp.where(allowed[None, None], jnp.exp(score), 0.0)
    denom = lax.optimization_barrier(jnp.sum(expo, axis=-1))
    weights = expo.astype(jnp.bfloat16).astype(jnp.float32)
    numer = jnp.einsum('gjrk,kgd->rgjd', weights, value_heads_split)
    denom = jnp.transpose(denom, (2, 0, 1))
    attn = numer / denom[:, :, :, None]
    return attn.reshape(element_count, HQ * HEAD_WIDTH).astype(jnp.bfloat16)

def finish(inputs, attn, output_weight, post_gain):
    proj = jnp.dot(attn, output_weight, preferred_element_type=jnp.float32)
    mean_sq = lax.optimization_barrier(jnp.mean(proj * proj, axis=-1, keepdims=True))
    return (inputs.astype(jnp.float32) + proj / jnp.sqrt(mean_sq + eps) * post_gain).astype(jnp.bfloat16)

def project(normed, weight):
    return jnp.dot(normed, weight, preferred_element_type=jnp.float32)

def reference(tokens, memory, norm_gain, post_gain, query_weight, key_matrix, value_matrix, output_weight, segment_weight):
    segs = N_SEG
    scale = 1.0 / HEAD_WIDTH ** 0.5
    seg_tokens = tokens.reshape(segs, TOK_DEV, MODEL_WIDTH)
    write_norm = prenorm(memory, norm_gain)
    write_q = (project(write_norm, query_weight) * scale).astype(jnp.bfloat16)
    write_k = project(write_norm, key_matrix).astype(jnp.bfloat16)
    write_v = project(write_norm, value_matrix).astype(jnp.bfloat16)

    def token_keys(rows):
        normed = prenorm(rows, norm_gain)
        return (project(normed, key_matrix).astype(jnp.bfloat16), project(normed, value_matrix).astype(jnp.bfloat16))
    tok_k, tok_v = lax.map(token_keys, seg_tokens)
    write_mask = jnp.concatenate([jnp.ones((MEM, MEM + TOK_DEV), bool), jnp.tril(jnp.ones((MEM, MEM), bool))], axis=1)

    def write_pass(items):
        read, keys_t, values_t = items
        normed = prenorm(read, norm_gain)
        read_k = project(normed, key_matrix).astype(jnp.bfloat16)
        read_v = project(normed, value_matrix).astype(jnp.bfloat16)
        key_vectors = jnp.concatenate([read_k, keys_t, write_k], axis=0)
        value_vectors = jnp.concatenate([read_v, values_t, write_v], axis=0)
        attn = attend(write_q, key_vectors, value_vectors, write_mask)
        return finish(memory, attn, output_weight, post_gain)
    read_all = jnp.broadcast_to(memory[None], (segs, MEM, MODEL_WIDTH))
    previous = read_all
    changes = []
    newest = previous
    read_used = read_all
    for step in range(ITERS):
        read_used = read_all
        newest = lax.map(write_pass, (read_all, tok_k, tok_v))
        diff = newest.astype(jnp.float32) - previous.astype(jnp.float32)
        per_segment = lax.optimization_barrier(jnp.sum(diff * diff, axis=(1, 2))) * segment_weight
        changes.append(jnp.sqrt(jnp.sum(per_segment) / (segs * MEM * MODEL_WIDTH) + eps))
        previous = newest
        read_all = jnp.concatenate([memory[None], newest[:-1]], axis=0)
    token_mask = jnp.concatenate([jnp.ones((TOK_DEV, MEM), bool), jnp.tril(jnp.ones((TOK_DEV, TOK_DEV), bool))], axis=1)

    def token_pass(items):
        rows, read, keys_t, values_t = items
        normed = prenorm(rows, norm_gain)
        query_vectors = (project(normed, query_weight) * scale).astype(jnp.bfloat16)
        read_norm = prenorm(read, norm_gain)
        read_k = project(read_norm, key_matrix).astype(jnp.bfloat16)
        read_v = project(read_norm, value_matrix).astype(jnp.bfloat16)
        key_vectors = jnp.concatenate([read_k, keys_t], axis=0)
        value_vectors = jnp.concatenate([read_v, values_t], axis=0)
        attn = attend(query_vectors, key_vectors, value_vectors, token_mask)
        return finish(rows, attn, output_weight, post_gain)
    token_out = lax.map(token_pass, (seg_tokens, read_used, tok_k, tok_v))
    return (token_out.reshape(segs * TOK_DEV, MODEL_WIDTH), newest.reshape(segs * MEM, MODEL_WIDTH), jnp.stack(changes).astype(jnp.float32))
```

```python
import functools

import jax
import jax.numpy as jnp
from jax import lax
from jax.experimental import pallas as pl
from jax.experimental.pallas import tpu as pltpu
from jax.sharding import PartitionSpec as P


HEAD_WIDTH = 256
KEY_VALUE_HEADS = 4
ITERS = 3
LANES = 128
MESH = pl.DeviceIdType.MESH


eps = 1e-06


def from_behind(block, axis, distance):
    devices = range(lax.axis_size(axis))
    route = [(i - distance, i) for i in devices if i - distance in devices]
    return lax.ppermute(block, axis, route)


def prenorm(rows, gain):
    rows = rows.astype(jnp.float32)
    mean_sq = jnp.mean(rows * rows, axis=-1, keepdims=True)
    return (rows / jnp.sqrt(mean_sq + eps) * gain).astype(jnp.bfloat16)


def reduce_kernel(n, part_ref, out_ref, held, total, send1, recv1, send2, recv2):
    me = lax.axis_index("seg")

    def scatter(k):
        to = lax.rem(me + k, n)
        return pltpu.make_async_remote_copy(
            src_ref=part_ref.at[to],
            dst_ref=held.at[k],
            send_sem=send1.at[k],
            recv_sem=recv1.at[k],
            device_id=(to,),
            device_id_type=MESH,
        )

    def spread(k):
        to = lax.rem(me + k, n)
        return pltpu.make_async_remote_copy(
            src_ref=total,
            dst_ref=out_ref.at[me],
            send_sem=send2.at[k],
            recv_sem=recv2.at[k],
            device_id=(to,),
            device_id_type=MESH,
        )

    @pl.loop(1, n)
    def _(k):
        scatter(k).start()

    total[...] = part_ref[me]

    @pl.loop(1, n)
    def _(k):
        scatter(k).wait_recv()
        total[...] += held[k]

    @pl.loop(1, n)
    def _(k):
        spread(k).start()

    out_ref[me] = total[...]

    @pl.loop(1, n)
    def _(k):
        scatter(k).wait_send()
        spread(k).wait()


def all_sum(parts):
    n = parts.shape[0]
    sems = pltpu.SemaphoreType.DMA((n,))
    return pl.pallas_call(
        functools.partial(reduce_kernel, n),
        out_shape=jax.ShapeDtypeStruct(parts.shape, parts.dtype),
        in_specs=[pl.BlockSpec(memory_space=pltpu.VMEM)],
        out_specs=pl.BlockSpec(memory_space=pltpu.VMEM),
        scratch_shapes=[
            pltpu.VMEM(parts.shape, parts.dtype),
            pltpu.VMEM(parts.shape[1:], parts.dtype),
            sems,
            sems,
            sems,
            sems,
        ],
        compiler_params=pltpu.CompilerParams(has_side_effects=True),
        cost_estimate=pl.CostEstimate(flops=0, bytes_accessed=30_000_000, transcendentals=0),
        name="query_sum",
    )(parts)


def total_kernel(n, part_ref, out_ref, held, send, recv):
    me = lax.axis_index("seg")

    def copy(k):
        return pltpu.make_async_remote_copy(
            src_ref=part_ref,
            dst_ref=held.at[me],
            send_sem=send.at[k],
            recv_sem=recv.at[k],
            device_id=(lax.rem(me + k, n),),
            device_id_type=MESH,
        )

    @pl.loop(1, n)
    def _(k):
        copy(k).start()

    held[me] = part_ref[...]

    @pl.loop(1, n)
    def _(k):
        copy(k).wait()

    out_ref[...] = jnp.sum(held[...], axis=0)


def small_sum(part, n):
    sems = pltpu.SemaphoreType.DMA((n,))
    return pl.pallas_call(
        functools.partial(total_kernel, n),
        out_shape=jax.ShapeDtypeStruct(part.shape, part.dtype),
        in_specs=[pl.BlockSpec(memory_space=pltpu.VMEM)],
        out_specs=pl.BlockSpec(memory_space=pltpu.VMEM),
        scratch_shapes=[pltpu.VMEM((n,) + part.shape, part.dtype), sems, sems],
        compiler_params=pltpu.CompilerParams(has_side_effects=True),
        cost_estimate=pl.CostEstimate(flops=0, bytes_accessed=8_000_000, transcendentals=0),
        name="change_sum",
    )(part)


def attend_kernel(first, keys, q_ref, rk_ref, rv_ref, k_ref, v_ref, out_ref):
    rows = q_ref.shape[0]
    nt = (((1,), (1,)), ((), ()))
    row = lax.broadcasted_iota(jnp.int32, (rows, keys), 0)
    col = lax.broadcasted_iota(jnp.int32, (rows, keys), 1)
    allowed = col <= row + first
    for half in range(2):
        cols = slice(half * HEAD_WIDTH, (half + 1) * HEAD_WIDTH)
        q = q_ref[:, cols]
        own = lax.dot_general(q, k_ref[:keys], nt, preferred_element_type=jnp.float32)
        own = jnp.where(allowed, jnp.exp(own), 0.0)
        read = jnp.exp(
            lax.dot_general(q, rk_ref[...], nt, preferred_element_type=jnp.float32)
        )
        denom = jnp.sum(own, axis=-1, keepdims=True) + jnp.sum(read, axis=-1, keepdims=True)
        numer = jnp.dot(
            own.astype(jnp.bfloat16), v_ref[:keys], preferred_element_type=jnp.float32
        ) + jnp.dot(read.astype(jnp.bfloat16), rv_ref[...], preferred_element_type=jnp.float32)
        out_ref[:, cols] = (numer / denom).astype(jnp.bfloat16)


def attend(q, read_k, read_v, local_k, local_v, first, keys):
    rows, width = q.shape
    mem, total = read_k.shape[0], local_k.shape[0]
    at = lambda h: (0, h)
    return pl.pallas_call(
        functools.partial(attend_kernel, first, keys),
        grid=(KEY_VALUE_HEADS,),
        out_shape=jax.ShapeDtypeStruct((rows, width), jnp.bfloat16),
        in_specs=[
            pl.BlockSpec((rows, 2 * HEAD_WIDTH), at),
            pl.BlockSpec((mem, HEAD_WIDTH), at),
            pl.BlockSpec((mem, HEAD_WIDTH), at),
            pl.BlockSpec((total, HEAD_WIDTH), at),
            pl.BlockSpec((total, HEAD_WIDTH), at),
        ],
        out_specs=pl.BlockSpec((rows, 2 * HEAD_WIDTH), at),
        cost_estimate=pl.CostEstimate(
            flops=4 * rows * width * (keys + mem), bytes_accessed=6_000_000, transcendentals=0
        ),
        name="attend",
    )(q, read_k, read_v, local_k, local_v)


def finish(inputs, attn, output_weight, post_gain):
    proj = jnp.dot(attn, output_weight, preferred_element_type=jnp.float32)
    mean_sq = jnp.mean(proj * proj, axis=-1, keepdims=True)
    return (inputs.astype(jnp.float32) + proj / jnp.sqrt(mean_sq + eps) * post_gain).astype(
        jnp.bfloat16
    )


def shards(
    tokens,
    memory,
    norm_gain,
    post_gain,
    query_weight,
    key_matrix,
    value_matrix,
    output_weight,
    segment_weight,
):
    n = lax.axis_size("seg")
    me = lax.axis_index("seg")
    tok_rows = tokens.shape[0]
    mem_rows, feature_width = memory.shape
    own_rows, query_width = query_weight.shape
    scale = 1.0 / HEAD_WIDTH**0.5
    output_full = lax.all_gather(output_weight, "seg", axis=0, tiled=True)

    mem_norm = prenorm(memory, norm_gain)
    own_cols = lax.dynamic_slice_in_dim(mem_norm, me * own_rows, own_rows, axis=1)
    part = jnp.dot(own_cols, query_weight, preferred_element_type=jnp.float32)
    blocks = query_width // LANES
    part = jnp.transpose(part.reshape(mem_rows, blocks, LANES), (1, 0, 2))
    summed = all_sum(part.reshape(n, mem_rows * blocks // n, LANES))
    summed = jnp.transpose(summed.reshape(blocks, mem_rows, LANES), (1, 0, 2))
    write_q = (summed.reshape(mem_rows, query_width) * scale).astype(jnp.bfloat16)

    own_query, write_q = lax.optimization_barrier((query_weight, write_q))
    query_full = lax.all_gather(own_query, "seg", axis=0, tiled=True)

    normed = prenorm(jnp.concatenate([tokens, memory], axis=0), norm_gain)
    local_k = jnp.dot(normed, key_matrix, preferred_element_type=jnp.float32).astype(jnp.bfloat16)
    local_v = jnp.dot(normed, value_matrix, preferred_element_type=jnp.float32).astype(jnp.bfloat16)
    total_rows = tok_rows + mem_rows
    first = jnp.int32(0) == me
    previous = memory
    squares = []
    own_weight = segment_weight[0]
    count_all = n * mem_rows * feature_width
    read_k, read_v = local_k[tok_rows:], local_v[tok_rows:]
    for step in range(ITERS):
        attn = attend(write_q, read_k, read_v, local_k, local_v, tok_rows, total_rows)
        newest = finish(memory, attn, output_full, post_gain)
        diff = newest.astype(jnp.float32) - previous.astype(jnp.float32)
        squares.append(jnp.sum(diff * diff) * own_weight)
        previous = newest
        if step + 1 < ITERS:
            read = jnp.where(first, memory, from_behind(newest, "seg", 1))
            read_norm = prenorm(read, norm_gain)
            read_k = jnp.dot(read_norm, key_matrix, preferred_element_type=jnp.float32).astype(
                jnp.bfloat16
            )
            read_v = jnp.dot(read_norm, value_matrix, preferred_element_type=jnp.float32).astype(
                jnp.bfloat16
            )
    squares = jnp.broadcast_to(jnp.pad(jnp.stack(squares), (0, LANES - ITERS))[None], (8, LANES))
    totals = small_sum(squares, n)[0, :ITERS]
    change_vec = jnp.sqrt(totals / count_all + eps)

    query_acc = jnp.dot(normed[:tok_rows], query_full, preferred_element_type=jnp.float32)
    query_vectors = (query_acc * scale).astype(jnp.bfloat16)
    attn = attend(query_vectors, read_k, read_v, local_k, local_v, 0, tok_rows)
    token_out = finish(tokens, attn, output_full, post_gain)
    return (token_out, previous, change_vec)


def solution(mesh):
    return jax.shard_map(
        shards,
        mesh=mesh,
        in_specs=(
            P("seg", None),
            P(),
            P(),
            P(),
            P("seg", None),
            P(),
            P(),
            P("seg", None),
            P("seg"),
        ),
        out_specs=(P("seg", None), P("seg", None), P()),
        check_vma=False,
    )
```

```python
import functools

import jax
import jax.numpy as jnp
from jax import lax
from jax.experimental import pallas as pl
from jax.experimental.pallas import tpu as pltpu
from jax.sharding import PartitionSpec as P


HEAD_WIDTH = 256
KEY_VALUE_HEADS = 4
ITERS = 3
LANES = 128
MESH = pl.DeviceIdType.MESH


eps = 1e-06


def from_behind(block, axis, distance):
    devices = range(lax.axis_size(axis))
    route = [(i - distance, i) for i in devices if i - distance in devices]
    return lax.ppermute(block, axis, route)


def prenorm(rows, gain):
    rows = rows.astype(jnp.float32)
    mean_sq = jnp.mean(rows * rows, axis=-1, keepdims=True)
    return (rows / jnp.sqrt(mean_sq + eps) * gain).astype(jnp.bfloat16)


def reduce_kernel(n, scale, part_ref, out_ref, held, total, final, send1, recv1, send2, recv2):
    me = lax.axis_index("seg") // 2
    core = lax.rem(lax.axis_index("seg"), 2)

    def scatter(k):
        to = lax.rem(me + k, n)
        return pltpu.make_async_remote_copy(
            src_ref=part_ref.at[to],
            dst_ref=held.at[k],
            send_sem=send1.at[k],
            recv_sem=recv1.at[k],
            device_id=(2 * to + core,),
            device_id_type=MESH,
        )

    def spread(k):
        to = lax.rem(me + k, n)
        return pltpu.make_async_remote_copy(
            src_ref=final,
            dst_ref=out_ref.at[me],
            send_sem=send2.at[k],
            recv_sem=recv2.at[k],
            device_id=(2 * to + core,),
            device_id_type=MESH,
        )

    @pl.loop(1, n)
    def _(k):
        scatter(k).start()

    total[...] = part_ref[me]

    @pl.loop(1, n)
    def _(k):
        scatter(k).wait_recv()
        total[...] += held[k]

    final[...] = (total[...] * scale).astype(final.dtype)

    @pl.loop(1, n)
    def _(k):
        spread(k).start()

    out_ref[me] = final[...]

    @pl.loop(1, n)
    def _(k):
        scatter(k).wait_send()
        spread(k).wait()


def all_sum(parts, scale):
    n = parts.shape[0]
    sems = pltpu.SemaphoreType.DMA((n,))
    return pl.pallas_call(
        functools.partial(reduce_kernel, n, scale),
        out_shape=jax.ShapeDtypeStruct(parts.shape, jnp.bfloat16),
        in_specs=[pl.BlockSpec(memory_space=pltpu.VMEM)],
        out_specs=pl.BlockSpec(memory_space=pltpu.VMEM),
        scratch_shapes=[
            pltpu.VMEM(parts.shape, parts.dtype),
            pltpu.VMEM(parts.shape[1:], parts.dtype),
            pltpu.VMEM(parts.shape[1:], jnp.bfloat16),
            sems,
            sems,
            sems,
            sems,
        ],
        compiler_params=pltpu.CompilerParams(has_side_effects=True),
        cost_estimate=pl.CostEstimate(flops=0, bytes_accessed=30_000_000, transcendentals=0),
        name="query_sum",
    )(parts)


def total_kernel(n, part_ref, out_ref, held, send, recv):
    me = lax.axis_index("seg")

    def copy(k):
        return pltpu.make_async_remote_copy(
            src_ref=part_ref,
            dst_ref=held.at[me],
            send_sem=send.at[k],
            recv_sem=recv.at[k],
            device_id=(lax.rem(me + k, n),),
            device_id_type=MESH,
        )

    @pl.loop(1, n)
    def _(k):
        copy(k).start()

    held[me] = part_ref[...]

    @pl.loop(1, n)
    def _(k):
        copy(k).wait()

    out_ref[...] = jnp.sum(held[...], axis=0)


def small_sum(part, n):
    sems = pltpu.SemaphoreType.DMA((n,))
    return pl.pallas_call(
        functools.partial(total_kernel, n),
        out_shape=jax.ShapeDtypeStruct(part.shape, part.dtype),
        in_specs=[pl.BlockSpec(memory_space=pltpu.VMEM)],
        out_specs=pl.BlockSpec(memory_space=pltpu.VMEM),
        scratch_shapes=[pltpu.VMEM((n,) + part.shape, part.dtype), sems, sems],
        compiler_params=pltpu.CompilerParams(has_side_effects=True),
        cost_estimate=pl.CostEstimate(flops=0, bytes_accessed=8_000_000, transcendentals=0),
        name="change_sum",
    )(part)


def attend_kernel(first, keys, q_ref, rk_ref, rv_ref, k_ref, v_ref, out_ref):
    rows = q_ref.shape[0]
    nt = (((1,), (1,)), ((), ()))
    row = lax.broadcasted_iota(jnp.int32, (rows, keys), 0)
    col = lax.broadcasted_iota(jnp.int32, (rows, keys), 1)
    allowed = col <= row + first
    for half in range(2):
        cols = slice(half * HEAD_WIDTH, (half + 1) * HEAD_WIDTH)
        q = q_ref[:, cols]
        own = lax.dot_general(q, k_ref[:keys], nt, preferred_element_type=jnp.float32)
        own = jnp.where(allowed, jnp.exp(own), 0.0)
        read = jnp.exp(
            lax.dot_general(q, rk_ref[...], nt, preferred_element_type=jnp.float32)
        )
        denom = jnp.sum(own, axis=-1, keepdims=True) + jnp.sum(read, axis=-1, keepdims=True)
        numer = jnp.dot(
            own.astype(jnp.bfloat16), v_ref[:keys], preferred_element_type=jnp.float32
        ) + jnp.dot(read.astype(jnp.bfloat16), rv_ref[...], preferred_element_type=jnp.float32)
        out_ref[:, cols] = (numer / denom).astype(jnp.bfloat16)


def attend(q, read_k, read_v, local_k, local_v, first, keys):
    rows, width = q.shape
    mem, total = read_k.shape[0], local_k.shape[0]
    at = lambda h: (0, h)
    return pl.pallas_call(
        functools.partial(attend_kernel, first, keys),
        grid=(KEY_VALUE_HEADS,),
        out_shape=jax.ShapeDtypeStruct((rows, width), jnp.bfloat16),
        in_specs=[
            pl.BlockSpec((rows, 2 * HEAD_WIDTH), at),
            pl.BlockSpec((mem, HEAD_WIDTH), at),
            pl.BlockSpec((mem, HEAD_WIDTH), at),
            pl.BlockSpec((total, HEAD_WIDTH), at),
            pl.BlockSpec((total, HEAD_WIDTH), at),
        ],
        out_specs=pl.BlockSpec((rows, 2 * HEAD_WIDTH), at),
        cost_estimate=pl.CostEstimate(
            flops=4 * rows * width * (keys + mem), bytes_accessed=6_000_000, transcendentals=0
        ),
        name="attend",
    )(q, read_k, read_v, local_k, local_v)


def finish(inputs, attn, output_weight, post_gain):
    proj = jnp.dot(attn, output_weight, preferred_element_type=jnp.float32)
    mean_sq = jnp.mean(proj * proj, axis=-1, keepdims=True)
    return (inputs.astype(jnp.float32) + proj / jnp.sqrt(mean_sq + eps) * post_gain).astype(
        jnp.bfloat16
    )


def shards(
    tokens,
    memory,
    norm_gain,
    post_gain,
    query_weight,
    key_matrix,
    value_matrix,
    output_weight,
    segment_weight,
):
    n = lax.axis_size("seg")
    me = lax.axis_index("seg")
    tok_rows = tokens.shape[0]
    mem_rows, feature_width = memory.shape
    own_rows, query_width = query_weight.shape
    scale = 1.0 / HEAD_WIDTH**0.5
    output_full = lax.all_gather(output_weight, "seg", axis=0, tiled=True)

    mem_norm = prenorm(memory, norm_gain)
    own_cols = lax.dynamic_slice_in_dim(mem_norm, me * own_rows, own_rows, axis=1)
    part = jnp.dot(own_cols, query_weight, preferred_element_type=jnp.float32)
    blocks = query_width // LANES
    part = jnp.transpose(part.reshape(mem_rows, blocks, LANES), (1, 0, 2))
    core = lax.rem(me, 2)
    pairs = [(i, i + 1 - 2 * (i % 2)) for i in range(n)]
    share = blocks // 2
    kept = lax.dynamic_slice_in_dim(part, core * share, share, axis=0)
    given = lax.dynamic_slice_in_dim(part, (1 - core) * share, share, axis=0)
    kept = kept + lax.ppermute(given, "seg", pairs)
    peers = n // 2
    own_q = all_sum(kept.reshape(peers, mem_rows * share // peers, LANES), scale)
    own_q = own_q.reshape(share, mem_rows, LANES)
    other_q = lax.ppermute(own_q, "seg", pairs)
    low = core == 0
    write_q = jnp.concatenate(
        [jnp.where(low, own_q, other_q), jnp.where(low, other_q, own_q)], axis=0
    )
    write_q = jnp.transpose(write_q, (1, 0, 2)).reshape(mem_rows, query_width)

    own_query, write_q = lax.optimization_barrier((query_weight, write_q))
    query_full = lax.all_gather(own_query, "seg", axis=0, tiled=True)

    normed = prenorm(jnp.concatenate([tokens, memory], axis=0), norm_gain)
    local_k = jnp.dot(normed, key_matrix, preferred_element_type=jnp.float32).astype(jnp.bfloat16)
    local_v = jnp.dot(normed, value_matrix, preferred_element_type=jnp.float32).astype(jnp.bfloat16)
    total_rows = tok_rows + mem_rows
    first = jnp.int32(0) == me
    previous = memory
    squares = []
    own_weight = segment_weight[0]
    count_all = n * mem_rows * feature_width
    read_k, read_v = local_k[tok_rows:], local_v[tok_rows:]
    for step in range(ITERS):
        attn = attend(write_q, read_k, read_v, local_k, local_v, tok_rows, total_rows)
        newest = finish(memory, attn, output_full, post_gain)
        diff = newest.astype(jnp.float32) - previous.astype(jnp.float32)
        squares.append(jnp.sum(diff * diff) * own_weight)
        previous = newest
        if step + 1 < ITERS:
            read = jnp.where(first, memory, from_behind(newest, "seg", 1))
            read_norm = prenorm(read, norm_gain)
            read_k = jnp.dot(read_norm, key_matrix, preferred_element_type=jnp.float32).astype(
                jnp.bfloat16
            )
            read_v = jnp.dot(read_norm, value_matrix, preferred_element_type=jnp.float32).astype(
                jnp.bfloat16
            )
    squares = jnp.broadcast_to(jnp.pad(jnp.stack(squares), (0, LANES - ITERS))[None], (8, LANES))
    totals = small_sum(squares, n)[0, :ITERS]
    change_vec = jnp.sqrt(totals / count_all + eps)

    query_acc = jnp.dot(normed[:tok_rows], query_full, preferred_element_type=jnp.float32)
    query_vectors = (query_acc * scale).astype(jnp.bfloat16)
    attn = attend(query_vectors, read_k, read_v, local_k, local_v, 0, tok_rows)
    token_out = finish(tokens, attn, output_full, post_gain)
    return (token_out, previous, change_vec)


def solution(mesh):
    return jax.shard_map(
        shards,
        mesh=mesh,
        in_specs=(
            P("seg", None),
            P(),
            P(),
            P(),
            P("seg", None),
            P(),
            P(),
            P("seg", None),
            P("seg"),
        ),
        out_specs=(P("seg", None), P("seg", None), P()),
        check_vma=False,
    )
```
